32 devices in a mesh: seq: 16 (over z, y, core), head: 2 (over x).
Axes of the slice: x: 2, y: 2, z: 4, core: 2. Of those that a mesh axis runs over, the one named last changes fastest.
Arguments:
- tokens: bfloat16 [1, 8192, 2048], P(None, 'seq'), may hold values from -6 to 6
- qkv_weight: bfloat16 [2048, 3, 2048], P(None, None, 'head'), may hold values from -1 to 1
- persistent: bfloat16 [2, 128, 2048], P(None, None, 'head'), may hold values from -60 to 60
- rate_weight: float32 [2048], replicated, may hold values from -0.25 to 0.25
- forget_rate: float32 [1, 8192], P(None, 'seq'), may hold values from 9.765625e-07 to 0.0009765625
- momentum_decay: float32 [1], replicated, may hold values from 0.5 to 0.95
- forget_share: float32 [1], replicated, may hold values from 0.05 to 0.5
- memory: float32 [2048, 2, 4096], P('seq', None, 'head'), may hold values from -0.125 to 0.125
- momentum: float32 [2048, 2, 4096], P('seq', None, 'head'), may hold values from -0.0625 to 0.0625
Outputs:
- attended: bfloat16 [1, 8192, 2048], P(None, 'seq', 'head')
- memory_out: float32 [2048, 2, 4096], P('seq', None, 'head')
- momentum_out: float32 [2048, 2, 4096], P('seq', None, 'head')
The draws below stay inside these ranges and needn't reach their ends.
All inputs are finite; a program needn't handle non-finite values.
Results may differ from the reference program's by a relative error of at most 0.01.
Values may be sent and summed in bfloat16 or wider, within the bound.
A program may use at most 128 MiB of HBM per device.

```python
import math
import jax
import jax.numpy as jnp
from jax import lax

D = 2048
HEADS = 16
HEAD_DIM = 128
MEM_UNITS = 4096
NP = 128
TOK_DEV = 512
BLOCKS = 1
TOKENS_STEP = 8192
N_SEQ = 16
N_HEAD = 2


def qkv_draw(key):
    raw_weights = jax.random.normal(jax.random.fold_in(key, 102), (D, 3, D), jnp.float32)
    return jnp.clip(raw_weights, -6.0, 6.0) * D ** (-0.5)


def draw_tokens(key, part):
    token_noise = jax.random.normal(jax.random.fold_in(key, 103), (BLOCKS, TOKENS_STEP, D), jnp.float32)
    values_all = token_noise
    return jnp.clip(values_all, -6.0, 6.0).astype(jnp.bfloat16)


def draw_qkv_weight(key, part):
    return qkv_draw(key).astype(jnp.bfloat16)


def draw_persistent(key, part):
    base_rows = jnp.clip(jax.random.normal(jax.random.fold_in(key, 104), (2, NP, D), jnp.float32), -6.0, 6.0)
    return base_rows.astype(jnp.bfloat16)


def level_of(own_key, shape, split, smallest, high):
    factor_of, own = 1.0, jax.random.fold_in(own_key, 6)
    for dim, blocks in split:
        draws = jnp.exp(jax.random.uniform(jax.random.fold_in(own, dim), (blocks,), jnp.float32, smallest / len(split), high / len(split)))
        factor_of = factor_of * jnp.repeat(draws, shape[dim] // blocks).reshape([-1 if axis == dim else 1 for axis in range(len(shape))])
    return factor_of


def centred(own_key, extent, deviation, reach, shards=(), kind=jnp.bfloat16):
    entries = jax.random.normal(own_key, extent, jnp.float32) * deviation
    if len(shards) > 0:
        entries = level_of(own_key, extent, shards, -0.22, 0.18) * entries
    return jnp.clip(entries, min=-reach, max=reach).astype(kind)


def setup_inputs(seed: int = 0) -> dict:
    key_of = jax.random.split(jax.random.key(seed), 10)
    tokens = draw_tokens(jax.random.fold_in(key_of[9], 71), 0)
    qkv_weight = draw_qkv_weight(jax.random.fold_in(key_of[9], 71), 0)
    persistent = draw_persistent(jax.random.fold_in(key_of[9], 71), 0)
    rate_weight = centred(key_of[3], (D,), (D // 4) ** -0.5, 0.25, (), jnp.float32)
    forget_rate = jnp.clip(jnp.exp(math.log(0.0009765625) - 6.9077552 * jax.random.uniform(key_of[4], (BLOCKS, TOKENS_STEP), jnp.float32) ** level_of(key_of[4], (BLOCKS, TOKENS_STEP), ((1, 16),), -0.2, 0.2)), 9.765625463842298e-07, 0.0009765625)
    momentum_decay = jnp.clip(jax.random.uniform(key_of[5], (BLOCKS,), jnp.float32, 0.5, 0.95), 0.5, 0.95)
    forget_share = jnp.clip(jax.random.uniform(key_of[6], (BLOCKS,), jnp.float32, 0.05, 0.5), 0.05, 0.5)
    memory = centred(key_of[7], (D, 2, MEM_UNITS), D ** -0.5, 0.125, ((0, 16), (2, 2)), jnp.float32)
    momentum = centred(key_of[8], (D, 2, MEM_UNITS), (4 * D) ** -0.5, 0.0625, ((0, 16), (2, 2)), jnp.float32)
    return {"tokens": tokens, "qkv_weight": qkv_weight, "persistent": persistent, "rate_weight": rate_weight, "forget_rate": forget_rate, "momentum_decay": momentum_decay, "forget_share": forget_share, "memory": memory, "momentum": momentum}


def key_mask(count, persist_count):
    rows_at = jnp.arange(count)[:, None]
    column = jnp.arange(persist_count + 2 * count)[None, :]
    local_pos = jnp.where(column < persist_count + count, column - persist_count, column - persist_count - count)
    return (column < persist_count) | (local_pos <= rows_at)


def attend_segment(parts, persist_keys, persist_values):
    query, keys, values, recalled = parts
    count = query.shape[0]
    all_keys = jnp.concatenate([persist_keys, recalled, keys], axis=0)
    all_values = jnp.concatenate([persist_values, recalled, values], axis=0)
    scores = jnp.einsum("thd,nhd->htn", query.astype(jnp.float32), all_keys.astype(jnp.float32)) * (HEAD_DIM ** -0.5)
    visible = key_mask(count, persist_keys.shape[0])
    scores = jnp.where(visible[None], scores, -1e30)
    largest = jnp.max(scores, axis=2, keepdims=True)
    expo = jnp.exp(scores - largest)
    probs = (expo / jnp.sum(expo, axis=2, keepdims=True)).astype(jnp.bfloat16)
    result = jnp.einsum("htn,nhd->thd", probs.astype(jnp.float32), all_values.astype(jnp.float32))
    return result.astype(jnp.bfloat16)


def reference(tokens, qkv_weight, persistent, rate_weight, forget_rate, momentum_decay, forget_share, memory, momentum):
    steps_len = TOKENS_STEP
    group = MEM_UNITS // N_HEAD
    lr_scale = 2.0 / (D * steps_len) ** 0.5
    tail = jnp.sum(forget_rate, axis=1, keepdims=True) - jnp.cumsum(forget_rate, axis=1)
    persist_keys = persistent[0].reshape(NP, HEADS, HEAD_DIM)
    persist_values = persistent[1].reshape(NP, HEADS, HEAD_DIM)
    results = []
    for block in range(BLOCKS):
        inputs = tokens[block]
        proj = jnp.einsum("td,dkf->tkf", inputs.astype(jnp.float32), qkv_weight.astype(jnp.float32)).astype(jnp.bfloat16)
        query, keys, values = proj[:, 0], proj[:, 1], proj[:, 2]
        weights_low = memory.astype(jnp.bfloat16)
        first, second = weights_low[:, 0, :], weights_low[:, 1, :]
        stacked = jnp.concatenate([query, keys], axis=0)
        preact = jnp.dot(stacked, first, preferred_element_type=jnp.float32)
        hidden = jax.nn.silu(preact).astype(jnp.bfloat16)
        summed = jnp.zeros((2 * steps_len, D), jnp.float32)
        for index in range(N_HEAD):
            piece = jnp.dot(hidden[:, index * group:(index + 1) * group], second[:, index * group:(index + 1) * group].T, preferred_element_type=jnp.float32).astype(jnp.bfloat16)
            piece = lax.optimization_barrier(piece)
            summed = summed + piece.astype(jnp.float32)
        recalled = summed[:steps_len].astype(jnp.bfloat16)
        errors = (summed[steps_len:] - values.astype(jnp.float32)).astype(jnp.bfloat16)

        def shaped(array):
            return array.reshape(N_SEQ, TOK_DEV, HEADS, HEAD_DIM)

        out_heads = lax.map(lambda parts: attend_segment(parts, persist_keys, persist_values), (shaped(query), shaped(keys), shaped(values), shaped(recalled)))
        results.append(out_heads.reshape(steps_len, D))
        rate = lr_scale * jax.nn.sigmoid(jnp.dot(inputs.astype(jnp.float32), rate_weight, precision=lax.Precision.HIGHEST))
        weight = rate * jnp.exp(-tail[block])
        key_pre = preact[steps_len:]
        key_hidden = hidden[steps_len:]
        sigm = jax.nn.sigmoid(key_pre)
        back = jnp.dot(errors, second, preferred_element_type=jnp.float32)
        dpre = back * sigm * (1.0 + key_pre * (1.0 - sigm))
        wdz = (weight[:, None] * dpre).astype(jnp.bfloat16)
        whid = (weight[:, None] * key_hidden.astype(jnp.float32)).astype(jnp.bfloat16)
        grad_first = jnp.dot(keys.T, wdz, preferred_element_type=jnp.float32)
        grad_second = jnp.dot(errors.T, whid, preferred_element_type=jnp.float32)
        grad = jnp.stack([grad_first, grad_second], axis=1)
        momentum = momentum_decay[block] * momentum - grad
        memory = (1.0 - forget_share[block]) * memory + momentum
    return jnp.stack(results, axis=0), memory, momentum
```

```python
import jax
import jax.numpy as jnp
from jax import lax
from jax.sharding import PartitionSpec as P

HEAD_DIM = 128
CHUNKS = 2


def later_total(total, axis):
    size, mine = (lax.axis_size(axis), lax.axis_index(axis))
    everything = lax.all_gather(total, axis)
    after = jnp.arange(size) > mine
    return jnp.sum(jnp.where(after, everything, 0.0))


def shifted(value, axis, by):
    size = lax.axis_size(axis)
    return lax.ppermute(value, axis, [(i, (i + by) % size) for i in range(size)])


def exchange(value, axis):
    return [shifted(value, axis, by) for by in range(1, lax.axis_size(axis))]


def in_order(own, others, axis):
    size, mine = (lax.axis_size(axis), lax.axis_index(axis))
    width = own.shape[1]
    if size == 2:
        return jnp.where(
            mine == 0,
            jnp.concatenate([own, others[0]], axis=1),
            jnp.concatenate([others[0], own], axis=1),
        )
    full = jnp.zeros((own.shape[0], width * size), own.dtype)
    full = lax.dynamic_update_slice(full, own, (0, mine * width))
    for by, other in enumerate(others, 1):
        full = lax.dynamic_update_slice(full, other, (0, lax.rem(mine + size - by, size) * width))
    return full


def key_mask(count, persist_count):
    rows_at = jnp.arange(count)[:, None]
    column = jnp.arange(persist_count + 2 * count)[None, :]
    local_pos = jnp.where(
        column < persist_count + count, column - persist_count, column - persist_count - count
    )
    return (column < persist_count) | (local_pos <= rows_at)


def attend_local(query, keys, values, recalled, persistent):
    count = query.shape[0]
    heads_here = query.shape[1] // HEAD_DIM
    persist_count = persistent.shape[1]
    persist_keys = persistent[0].reshape(persist_count, heads_here, HEAD_DIM)
    persist_values = persistent[1].reshape(persist_count, heads_here, HEAD_DIM)
    recall_heads = recalled.reshape(count, heads_here, HEAD_DIM)
    all_keys = jnp.concatenate(
        [persist_keys, recall_heads, keys.reshape(count, heads_here, HEAD_DIM)], axis=0
    )
    all_values = jnp.concatenate(
        [persist_values, recall_heads, values.reshape(count, heads_here, HEAD_DIM)], axis=0
    )
    scores = jnp.einsum(
        "thd,nhd->htn",
        query.reshape(count, heads_here, HEAD_DIM),
        all_keys,
        preferred_element_type=jnp.float32,
    ) * HEAD_DIM ** (-0.5)
    visible = key_mask(count, persist_count)
    scores = jnp.where(visible[None], scores, -1e30)
    largest = jnp.max(scores, axis=2, keepdims=True)
    expo = jnp.exp(scores - largest)
    probs = (expo / jnp.sum(expo, axis=2, keepdims=True)).astype(jnp.bfloat16)
    result = jnp.einsum("htn,nhd->thd", probs, all_values, preferred_element_type=jnp.float32)
    return result.astype(jnp.bfloat16).reshape(count, heads_here * HEAD_DIM)


def matmul(a, b):
    return jnp.dot(a, b, preferred_element_type=jnp.float32)


def times_transposed(a, b):
    return lax.dot_general(a, b, (((1,), (1,)), ((), ())), preferred_element_type=jnp.float32)


def transposed_times(a, b):
    return lax.dot_general(a, b, (((0,), (0,)), ((), ())), preferred_element_type=jnp.float32)


def on_device(
    tokens,
    qkv_weight,
    persistent,
    rate_weight,
    forget_rate,
    momentum_decay,
    forget_share,
    memory,
    momentum,
):
    seg_len = tokens.shape[1]
    width = tokens.shape[2]
    n_seq, n_head = lax.axis_size("seq"), lax.axis_size("head")
    head = lax.axis_index("head")
    rows = memory.shape[0]
    part = rows // CHUNKS
    here = width // n_head
    blocks = here // rows
    assert blocks * rows == here and part * CHUNKS == rows
    lr_scale = 2.0 / (width * n_seq * seg_len) ** 0.5

    gather = lambda rows_here: lax.all_gather(
        rows_here.astype(jnp.bfloat16), "seq", axis=0, tiled=True
    )
    first_here = memory[:, 0, :].astype(jnp.bfloat16)
    inputs = tokens[0]
    first_here, inputs = lax.optimization_barrier((first_here, inputs))
    first = gather(first_here)
    second = [gather(memory[c * part : (c + 1) * part, 1, :]) for c in range(CHUNKS)]

    project = lambda k: matmul(inputs, qkv_weight[:, k, :]).astype(jnp.bfloat16)
    keys = project(1)
    keys_others = exchange(keys, "head")
    query = project(0)
    query_others = exchange(query, "head")
    values = project(2)

    total = jnp.sum(forget_rate)
    later = later_total(total, "seq")
    tail = total - jnp.cumsum(forget_rate[0]) + later
    rate = lr_scale * jax.nn.sigmoid(
        jnp.dot(inputs.astype(jnp.float32), rate_weight, precision=lax.Precision.HIGHEST)
    )
    weight = rate * jnp.exp(-tail)

    keys_full = in_order(keys, keys_others, "head")
    query_full = in_order(query, query_others, "head")
    keys_full, weight, first = lax.optimization_barrier((keys_full, weight, first))
    key_pre = matmul(keys_full, first)
    key_hidden = jax.nn.silu(key_pre).astype(jnp.bfloat16)
    second[0], query_full = lax.optimization_barrier((second[0], query_full))
    query_hidden = jax.nn.silu(matmul(query_full, first)).astype(jnp.bfloat16)
    second[-1], query_hidden = lax.optimization_barrier((second[-1], query_hidden))
    whid = (weight[:, None] * key_hidden.astype(jnp.float32)).astype(jnp.bfloat16)

    values_split = values.reshape(seg_len, blocks, CHUNKS, part)
    back = 0.0
    errors = []
    grads_second = []
    for c in range(CHUNKS):
        minus = lax.dynamic_update_slice(
            jnp.zeros((seg_len, n_seq * part), jnp.bfloat16),
            values_split[:, :, c].reshape(seg_len, blocks * part),
            (0, head * blocks * part),
        )
        sent = (times_transposed(key_hidden, second[c]) - minus.astype(jnp.float32)).astype(
            jnp.bfloat16
        )
        others = exchange(sent, "head")
        error = sent.astype(jnp.float32)
        for other in others:
            error = error + other.astype(jnp.float32)
        error = error.astype(jnp.bfloat16)
        errors.append(error)
        grad = transposed_times(error, whid).astype(jnp.bfloat16)
        grads_second.append(lax.psum_scatter(grad, "seq", scatter_dimension=0, tiled=True))
        back = back + matmul(error, second[c])

    sigm = jax.nn.sigmoid(key_pre)
    dpre = back * sigm * (1.0 + key_pre * (1.0 - sigm))
    wdz = (weight[:, None] * dpre).astype(jnp.bfloat16)
    grad = transposed_times(keys_full, wdz).astype(jnp.bfloat16)
    grad_first = lax.psum_scatter(grad, "seq", scatter_dimension=0, tiled=True)

    query_hidden, _ = lax.optimization_barrier((query_hidden, errors[-1]))
    recalled = []
    for c in range(CHUNKS):
        partial = times_transposed(query_hidden, second[c]).astype(jnp.bfloat16)
        columns = lambda at: lax.dynamic_slice(
            partial, (0, at * blocks * part), (seg_len, blocks * part)
        )
        mine = columns(head).astype(jnp.float32)
        for by in range(1, n_head):
            other = shifted(columns(lax.rem(head + by, n_head)), "head", by)
            mine = mine + other.astype(jnp.float32)
        recalled.append(mine.astype(jnp.bfloat16).reshape(seg_len, blocks, part))
    recalled = jnp.stack(recalled, axis=2).reshape(seg_len, here)
    attended = attend_local(query, keys, values, recalled, persistent)

    grad = jnp.stack([grad_first, jnp.concatenate(grads_second, axis=0)], axis=1).astype(jnp.float32)
    momentum = momentum_decay[0] * momentum - grad
    memory = (1.0 - forget_share[0]) * memory + momentum
    return (attended[None], memory, momentum)


def solution(mesh):
    placed = (
        P(None, "seq", None),
        P(None, None, "head"),
        P(None, None, "head"),
        P(),
        P(None, "seq"),
        P(),
        P(),
        P("seq", None, "head"),
        P("seq", None, "head"),
    )
    return jax.shard_map(
        on_device,
        mesh=mesh,
        in_specs=placed,
        out_specs=(P(None, "seq", "head"), P("seq", None, "head"), P("seq", None, "head")),
        check_vma=False,
    )
```

```python
import jax
import jax.numpy as jnp
from jax import lax
from jax.sharding import PartitionSpec as P

HEAD_DIM = 128
CHUNKS = 2


def later_total(total, axis):
    size, mine = (lax.axis_size(axis), lax.axis_index(axis))
    everything = lax.all_gather(total, axis)
    after = jnp.arange(size) > mine
    return jnp.sum(jnp.where(after, everything, 0.0))


def shifted(value, axis, by):
    size = lax.axis_size(axis)
    return lax.ppermute(value, axis, [(i, (i + by) % size) for i in range(size)])


def exchange(value, axis):
    return [shifted(value, axis, by) for by in range(1, lax.axis_size(axis))]


def halves(held, axis, bit):
    pairs = held.reshape(held.shape[0] // 2, 2, held.shape[1], held.shape[2])
    side = lax.rem(lax.axis_index(axis) // bit, 2)
    keep = lax.dynamic_index_in_dim(pairs, side, 1, False)
    send = lax.dynamic_index_in_dim(pairs, 1 - side, 1, False)
    return (keep, send)


def partner_sum(keep, send, axis, bit):
    got = lax.ppermute(send, axis, [(i, i ^ bit) for i in range(lax.axis_size(axis))])
    return keep.astype(jnp.float32) + got.astype(jnp.float32)


def by_destination(grad, axis):
    size = lax.axis_size(axis)
    assert size & (size - 1) == 0
    return grad.reshape(size, grad.shape[0] // size, grad.shape[1])


def scatter_from(held, axis, bit, stop):
    while bit < stop:
        held = partner_sum(*halves(held.astype(jnp.bfloat16), axis, bit), axis, bit)
        bit *= 2
    return held


def in_order(own, others, axis):
    size, mine = (lax.axis_size(axis), lax.axis_index(axis))
    width = own.shape[1]
    if size == 2:
        return jnp.where(
            mine == 0,
            jnp.concatenate([own, others[0]], axis=1),
            jnp.concatenate([others[0], own], axis=1),
        )
    full = jnp.zeros((own.shape[0], width * size), own.dtype)
    full = lax.dynamic_update_slice(full, own, (0, mine * width))
    for by, other in enumerate(others, 1):
        full = lax.dynamic_update_slice(full, other, (0, lax.rem(mine + size - by, size) * width))
    return full


def key_mask(count, persist_count):
    rows_at = jnp.arange(count)[:, None]
    column = jnp.arange(persist_count + 2 * count)[None, :]
    local_pos = jnp.where(
        column < persist_count + count, column - persist_count, column - persist_count - count
    )
    return (column < persist_count) | (local_pos <= rows_at)


def attend_local(query, keys, values, recalled, persistent):
    count = query.shape[0]
    heads_here = query.shape[1] // HEAD_DIM
    persist_count = persistent.shape[1]
    persist_keys = persistent[0].reshape(persist_count, heads_here, HEAD_DIM)
    persist_values = persistent[1].reshape(persist_count, heads_here, HEAD_DIM)
    recall_heads = recalled.reshape(count, heads_here, HEAD_DIM)
    all_keys = jnp.concatenate(
        [persist_keys, recall_heads, keys.reshape(count, heads_here, HEAD_DIM)], axis=0
    )
    all_values = jnp.concatenate(
        [persist_values, recall_heads, values.reshape(count, heads_here, HEAD_DIM)], axis=0
    )
    scores = jnp.einsum(
        "thd,nhd->htn",
        query.reshape(count, heads_here, HEAD_DIM),
        all_keys,
        preferred_element_type=jnp.float32,
    ) * HEAD_DIM ** (-0.5)
    visible = key_mask(count, persist_count)
    scores = jnp.where(visible[None], scores, -1e30)
    largest = jnp.max(scores, axis=2, keepdims=True)
    expo = jnp.exp(scores - largest)
    probs = (expo / jnp.sum(expo, axis=2, keepdims=True)).astype(jnp.bfloat16)
    result = jnp.einsum("htn,nhd->thd", probs, all_values, preferred_element_type=jnp.float32)
    return result.astype(jnp.bfloat16).reshape(count, heads_here * HEAD_DIM)


def matmul(a, b):
    return jnp.dot(a, b, preferred_element_type=jnp.float32)


def times_transposed(a, b):
    return lax.dot_general(a, b, (((1,), (1,)), ((), ())), preferred_element_type=jnp.float32)


def transposed_times(a, b):
    return lax.dot_general(a, b, (((0,), (0,)), ((), ())), preferred_element_type=jnp.float32)


def on_device(
    tokens,
    qkv_weight,
    persistent,
    rate_weight,
    forget_rate,
    momentum_decay,
    forget_share,
    memory,
    momentum,
):
    seg_len = tokens.shape[1]
    width = tokens.shape[2]
    n_seq, n_head = lax.axis_size("seq"), lax.axis_size("head")
    head = lax.axis_index("head")
    rows = memory.shape[0]
    part = rows // CHUNKS
    here = width // n_head
    blocks = here // rows
    assert blocks * rows == here and part * CHUNKS == rows
    lr_scale = 2.0 / (width * n_seq * seg_len) ** 0.5

    inputs = tokens[0]
    weights_here, inputs = lax.optimization_barrier((memory.astype(jnp.bfloat16), inputs))
    weights = lax.all_gather(weights_here, "seq", axis=0, tiled=True)

    project = lambda k: matmul(inputs, qkv_weight[:, k, :]).astype(jnp.bfloat16)
    keys = project(1)
    keys_others = exchange(keys, "head")
    query = project(0)
    query_others = exchange(query, "head")
    values = project(2)

    total = jnp.sum(forget_rate)
    later = later_total(total, "seq")
    tail = total - jnp.cumsum(forget_rate[0]) + later
    rate = lr_scale * jax.nn.sigmoid(
        jnp.dot(inputs.astype(jnp.float32), rate_weight, precision=lax.Precision.HIGHEST)
    )
    weight = rate * jnp.exp(-tail)

    keys_full = in_order(keys, keys_others, "head")
    query_full = in_order(query, query_others, "head")
    keys_full, query_full, weight, weights = lax.optimization_barrier(
        (keys_full, query_full, weight, weights)
    )
    first = weights[:, 0, :]
    second = weights[:, 1, :].reshape(n_seq, CHUNKS, part, -1)
    second = [second[:, c].reshape(n_seq * part, -1) for c in range(CHUNKS)]
    key_pre = matmul(keys_full, first)
    key_hidden = jax.nn.silu(key_pre).astype(jnp.bfloat16)
    whid = (weight[:, None] * key_hidden.astype(jnp.float32)).astype(jnp.bfloat16)

    values_split = values.reshape(seg_len, blocks, CHUNKS, part)
    errors = []
    opened = []
    for c in range(CHUNKS):
        minus = lax.dynamic_update_slice(
            jnp.zeros((seg_len, n_seq * part), jnp.bfloat16),
            values_split[:, :, c].reshape(seg_len, blocks * part),
            (0, head * blocks * part),
        )
        sent = (times_transposed(key_hidden, second[c]) - minus.astype(jnp.float32)).astype(
            jnp.bfloat16
        )
        others = exchange(sent, "head")
        error = sent.astype(jnp.float32)
        for other in others:
            error = error + other.astype(jnp.float32)
        error = error.astype(jnp.bfloat16)
        errors.append(error)
        grad = transposed_times(error, whid).astype(jnp.bfloat16)
        opened.append(halves(by_destination(grad, "seq"), "seq", 1))
    errors, opened = lax.optimization_barrier((errors, opened))
    back = sum(matmul(error, rows_of) for error, rows_of in zip(errors, second))

    sigm = jax.nn.sigmoid(key_pre)
    dpre = back * sigm * (1.0 + key_pre * (1.0 - sigm))
    wdz = (weight[:, None] * dpre).astype(jnp.bfloat16)
    late = []
    for columns in jnp.split(wdz, CHUNKS, axis=1):
        grad = transposed_times(keys_full, columns).astype(jnp.bfloat16)
        late.append(halves(by_destination(grad, "seq"), "seq", 1))
    early = min(4, n_seq)
    opened = [partner_sum(*pair, "seq", 1).astype(jnp.bfloat16) for pair in opened]
    late, opened, query_full = lax.optimization_barrier((late, opened, query_full))
    late = [partner_sum(*pair, "seq", 1) for pair in late]
    summed = [scatter_from(held, "seq", 2, early) for held in opened + late]

    query_hidden = jax.nn.silu(matmul(query_full, first)).astype(jnp.bfloat16)
    recalled = []
    for c in range(CHUNKS):
        partial = times_transposed(query_hidden, second[c]).astype(jnp.bfloat16)
        columns = lambda at: lax.dynamic_slice(
            partial, (0, at * blocks * part), (seg_len, blocks * part)
        )
        mine = columns(head).astype(jnp.float32)
        for by in range(1, n_head):
            other = shifted(columns(lax.rem(head + by, n_head)), "head", by)
            mine = mine + other.astype(jnp.float32)
        recalled.append(mine.astype(jnp.bfloat16).reshape(seg_len, blocks, part))
    recalled = jnp.stack(recalled, axis=2).reshape(seg_len, here)

    heads = here // HEAD_DIM
    groups = len(summed) if heads % len(summed) == 0 else 1
    wide = here // groups
    attended = []
    for g in range(groups):
        at = slice(g * wide, (g + 1) * wide)
        if early < n_seq:
            pair = halves(summed[g].astype(jnp.bfloat16), "seq", early)
            pair, piece = lax.optimization_barrier((pair, query[:, at]))
            summed[g] = partner_sum(*pair, "seq", early)
        else:
            piece = query[:, at]
        attended.append(
            attend_local(piece, keys[:, at], values[:, at], recalled[:, at], persistent[:, :, at])
        )
    attended = jnp.concatenate(attended, axis=1)
    done = [
        scatter_from(held, "seq", 2 * early if g < groups else early, n_seq)[0]
        for g, held in enumerate(summed)
    ]
    grad = jnp.stack(
        [jnp.concatenate(done[CHUNKS:], axis=1), jnp.concatenate(done[:CHUNKS], axis=0)], axis=1
    )
    momentum = momentum_decay[0] * momentum - grad
    memory = (1.0 - forget_share[0]) * memory + momentum
    return (attended[None], memory, momentum)


def solution(mesh):
    placed = (
        P(None, "seq", None),
        P(None, None, "head"),
        P(None, None, "head"),
        P(),
        P(None, "seq"),
        P(),
        P(),
        P("seq", None, "head"),
        P("seq", None, "head"),
    )
    return jax.shard_map(
        on_device,
        mesh=mesh,
        in_specs=placed,
        out_specs=(P(None, "seq", "head"), P("seq", None, "head"), P("seq", None, "head")),
        check_vma=False,
    )
```
